128 devices in a mesh: py: 4 (over z_hi, core), px: 8 (over z_lo, x), pz: 4 (over y).
Axes of the slice: x: 4, y: 4, z: 4 (z_hi: 2, z_lo: 2; z = z_hi * 2 + z_lo), core: 2. Of those that a mesh axis runs over, the one named last changes fastest.
Arguments:
- density: float32 [32, 512, 128, 128], P('py', 'px', 'pz'), may hold values from 0.2 to 1.8
- crowding: float32 [32, 512, 128, 128], P('py', 'px', 'pz'), may hold values from 0.5 to 2
Outputs:
- column_sum: float32 [32, 512, 128, 128], P('py', 'px', 'pz')
- density_end: float32 [32, 512, 128, 128], P('py', 'px', 'pz')
The draws below stay inside these ranges and needn't reach their ends.
All inputs are finite; a program needn't handle non-finite values.
Results may differ from the reference program's by a relative error of at most 0.00002.
Values sent between devices are 32-bit elements; how exact they have to be, the bound alone decides.
A program may use at most 320 MiB of HBM per device.

```python
import jax
import jax.numpy as jnp
from jax import lax

GRID_Y = 32
GRID_X = 512
GRID_Z = 128
SPECIES = 128
STEPS = 6


def block_scale(stream_key, extent, cuts, low, largest):
    gain, own = 1.0, jax.random.fold_in(stream_key, 6)
    for position, parts in cuts:
        heights = jnp.exp(jax.random.uniform(jax.random.fold_in(own, position), (parts,), jnp.float32, low / len(cuts), largest / len(cuts)))
        gain = gain * jnp.repeat(heights, extent[position] // parts).reshape([-1 if axis == position else 1 for axis in range(len(extent))])
    return gain


def setup_inputs(seed: int = 0) -> dict:
    streams_of = jax.random.split(jax.random.key(seed), 3)
    return {
        "density": jnp.clip(0.2 + 1.5999999 * jax.random.uniform(streams_of[0], (GRID_Y, GRID_X, GRID_Z, SPECIES), jnp.float32) ** block_scale(streams_of[0], (GRID_Y, GRID_X, GRID_Z, SPECIES), ((0, 4), (1, 8), (2, 4)), -0.2, 0.2), 0.2, 1.8),
        "crowding": jnp.clip(0.5 + 1.5 * jax.random.uniform(streams_of[1], (GRID_Y, GRID_X, GRID_Z, SPECIES), jnp.float32) ** block_scale(streams_of[1], (GRID_Y, GRID_X, GRID_Z, SPECIES), ((0, 4), (1, 8), (2, 4)), -0.2, 0.2), 0.5, 2.0),
    }


def without_rim(values, dims):
    for dim in dims:
        values = lax.slice_in_dim(values, 1, values.shape[dim] - 1, axis=dim)
    return values


def shifted_cells(values, dim, start, dims):
    others = [other for other in dims if other != dim]
    values = without_rim(values, others)
    return lax.slice_in_dim(values, start, start + values.shape[dim] - 2, axis=dim)


def march_step(padded, crowding):
    middle = without_rim(padded, (0, 1, 2))
    lower = [shifted_cells(padded, dim, 0, (0, 1, 2)) for dim in (0, 1, 2)]
    upper = [shifted_cells(padded, dim, 2, (0, 1, 2)) for dim in (0, 1, 2)]
    spread = lower[0] + upper[0] + lower[1] + upper[1] + lower[2] + upper[2] - 6.0 * middle
    return middle + 0.1 * spread + 0.2 * middle * (1.0 - middle * crowding)


def reference(density, crowding):
    for step in range(STEPS):
        density = march_step(jnp.pad(density, ((1, 1), (1, 1), (1, 1), (0, 0)), mode="constant"), crowding)
    column_sum = jnp.cumsum(density, axis=0) / GRID_Y
    return column_sum, density
```

```python
import functools

import jax
import jax.numpy as jnp
from jax import lax
from jax.experimental import pallas as pl
from jax.experimental.pallas import tpu as pltpu
from jax.sharding import PartitionSpec as P

STEPS = 6
CHUNKS = 8
MESH = pl.DeviceIdType.MESH
LOW, HIGH = 8, 40


def kernel(sizes, d_ref, c_ref, col_ref, end_ref, field, crowd, below, total,
           in_sem, c_sem, y_send, y_recv, z_send, z_recv, x_send, x_recv, t_send, t_recv):
    ny, nx, nz = sizes
    py, px, pz = lax.axis_index("py"), lax.axis_index("px"), lax.axis_index("pz")
    Y, X, Z, _ = d_ref.shape
    width = X // CHUNKS
    even = lax.rem(px, 2) == 0

    def start_of(k):
        return pl.multiple_of(jnp.where(even, k, CHUNKS - 1 - k) * width, width)

    y_up = (py < ny - 1, {"py": py + 1, "px": px, "pz": pz})
    y_down = (py > 0, {"py": py - 1, "px": px, "pz": pz})
    z_up = (pz < nz - 1, {"py": py, "px": px, "pz": pz + 1})
    z_down = (pz > 0, {"py": py, "px": px, "pz": pz - 1})
    first = jnp.where(even, px - 1, px + 1)
    last = jnp.where(even, px + 1, px - 1)
    x_first = ((first >= 0) & (first < nx), {"py": py, "px": first, "pz": pz})
    x_last = ((last >= 0) & (last < nx), {"py": py, "px": last, "pz": pz})
    neighbours = (y_up, y_down, z_up, z_down, x_first, x_last)

    def load(k):
        x0 = start_of(k)
        return (
            pltpu.make_async_copy(
                d_ref.at[:, pl.ds(x0, width)],
                field.at[0, pl.ds(1, Y), pl.ds(1 + x0, width), pl.ds(LOW, Z)],
                in_sem.at[k],
            ),
            pltpu.make_async_copy(c_ref.at[:, pl.ds(x0, width)], crowd.at[:, pl.ds(x0, width)], c_sem.at[k]),
        )

    for k in range(CHUNKS):
        load(k)[0].start()
    for k in range(CHUNKS):
        load(k)[1].start()

    zero_row = jnp.zeros((1, 128), jnp.float32)
    zero_plane = jnp.zeros((Z, 128), jnp.float32)

    def clear_rows(row):
        def one(i, _):
            y, x = 1 + i // X, 1 + lax.rem(i, X)
            for p in range(2):
                field[p, y, x, pl.ds(row, 1), :] = zero_row
            return 0

        lax.fori_loop(0, Y * X, one, 0)

    def clear_plane(y):
        def one(x, _):
            for p in range(2):
                field[p, y, 1 + x, pl.ds(LOW, Z), :] = zero_plane
            return 0

        lax.fori_loop(0, X, one, 0)

    def clear_column(x):
        def one(y, _):
            for p in range(2):
                field[p, 1 + y, x, pl.ds(LOW, Z), :] = zero_plane
            return 0

        lax.fori_loop(0, Y, one, 0)

    pl.when(pz == 0)(lambda: clear_rows(LOW - 1))
    pl.when(pz == nz - 1)(lambda: clear_rows(HIGH))
    pl.when(py == 0)(lambda: clear_plane(0))
    pl.when(py == ny - 1)(lambda: clear_plane(Y + 1))
    pl.when(px == 0)(lambda: clear_column(0))
    pl.when(px == nx - 1)(lambda: clear_column(X + 1))

    barrier = pltpu.get_barrier_semaphore()
    count = 0
    for exists, device in neighbours:
        count = count + exists.astype(jnp.int32)

        @pl.when(exists)
        def _():
            pl.semaphore_signal(barrier, inc=1, device_id=device, device_id_type=MESH)

    pl.semaphore_wait(barrier, count)

    def remote(src, dst, send, recv, device):
        return pltpu.make_async_remote_copy(src, dst, send, recv, device_id=device, device_id_type=MESH)

    def faces(p, k):
        xs = pl.ds(1 + start_of(k), width)
        ys, zs = pl.ds(1, Y), pl.ds(LOW, Z)
        f = field.at[p]
        return (
            (y_up[0], remote(f.at[Y, xs, zs], f.at[0, xs, zs], y_send.at[p, 0, k], y_recv.at[p, 0, k], y_up[1])),
            (y_down[0], remote(f.at[1, xs, zs], f.at[Y + 1, xs, zs], y_send.at[p, 1, k], y_recv.at[p, 1, k], y_down[1])),
            (z_up[0], remote(f.at[ys, xs, pl.ds(HIGH - 1, 1)], f.at[ys, xs, pl.ds(LOW - 1, 1)], z_send.at[p, 0, k], z_recv.at[p, 0, k], z_up[1])),
            (z_down[0], remote(f.at[ys, xs, pl.ds(LOW, 1)], f.at[ys, xs, pl.ds(HIGH, 1)], z_send.at[p, 1, k], z_recv.at[p, 1, k], z_down[1])),
        )

    def ends(p, side):
        ys, zs = pl.ds(1, Y), pl.ds(LOW, Z)
        f = field.at[p]
        low = even if side == 0 else jnp.logical_not(even)
        src, dst = jnp.where(low, 1, X), jnp.where(low, X + 1, 0)
        exists, device = x_first if side == 0 else x_last
        return exists, remote(f.at[ys, pl.ds(src, 1), zs], f.at[ys, pl.ds(dst, 1), zs], x_send.at[p, side], x_recv.at[p, side], device)

    def each(p, k, do_faces, do_ends):
        arrivals = (1, 0, 3, 2)
        fs = faces(p, k)
        for i, (exists, copy) in enumerate(fs):
            do_faces(exists, copy, fs[arrivals[i]][0])
        for side, at in ((0, 0), (1, CHUNKS - 1)):
            exists, copy = ends(p, side)
            pl.when(exists & (k == at))(lambda copy=copy: do_ends(copy))

    def send(p, k):
        each(p, k, lambda e, c, _: pl.when(e)(lambda: c.start()), lambda c: c.start())

    def sent(p, k):
        each(p, k, lambda e, c, _: pl.when(e)(lambda: c.wait_send()), lambda c: c.wait_send())

    def arrived(p, k):
        each(p, k, lambda _, c, e: pl.when(e)(lambda: c.wait_recv()), lambda c: c.wait_recv())

    def cells(p, y, x, z):
        return field[p, y, x, pl.ds(z, 8), :]

    def chunk(t, k, store):
        p = t % 2
        x0 = start_of(k)

        def column(i, _):
            x = x0 + i
            for z in range(LOW, HIGH, 8):
                line = [cells(p, y, 1 + x, z) for y in range(Y + 2)]
                out = []
                for y in range(1, Y + 1):
                    middle = line[y]
                    crowding = crowd[y - 1, x, pl.ds(z - LOW, 8), :]
                    near = (line[y - 1] + line[y + 1]) + (cells(p, y, x, z) + cells(p, y, x + 2, z))
                    near = near + (cells(p, y, 1 + x, z - 1) + cells(p, y, 1 + x, z + 1))
                    out.append(0.1 * (middle * (6.0 - 2.0 * crowding * middle) + near))
                store(x, z, out)
            return 0

        lax.fori_loop(0, width, column, 0)

    def first_send(k, _):
        load(k)[0].wait()
        send(0, k)
        return 0

    lax.fori_loop(0, CHUNKS, first_send, 0)

    for t in range(STEPS - 1):
        q = (t + 1) % 2

        def store(x, z, out):
            for y in range(Y):
                field[q, 1 + y, 1 + x, pl.ds(z, 8), :] = out[y]

        def step(k, _):
            arrived(t % 2, k)
            if t == 0:
                load(k)[1].wait()
            else:
                sent(q, k)
            chunk(t, k, store)
            send(q, k)
            return 0

        lax.fori_loop(0, CHUNKS, step, 0)

    def finish(x, z, out):
        here = None
        for y in range(Y):
            end_ref[y, x, pl.ds(z - LOW, 8), :] = out[y]
            here = out[y] if here is None else here + out[y]
            col_ref[y, x, pl.ds(z - LOW, 8), :] = here
        total[x, pl.ds(z - LOW, 8), :] = here

    def pass_on(k):
        xs = pl.ds(start_of(k), width)
        return remote(total.at[xs], below.at[xs], t_send.at[k], t_recv.at[k], y_up[1])

    def prefix(k):
        x0 = start_of(k)

        @pl.when(py > 0)
        def _():
            pass_on(k).wait_recv()

            def add(i, _):
                total[x0 + i] = total[x0 + i] + below[x0 + i]
                return 0

            lax.fori_loop(0, width, add, 0)

        @pl.when(py < ny - 1)
        def _():
            pass_on(k).start()

        scale = 1.0 / (Y * ny)

        def complete(i, _):
            lower = jnp.where(py > 0, below[x0 + i], 0.0)
            for y in range(Y):
                col_ref[y, x0 + i] = (col_ref[y, x0 + i] + lower) * scale
            return 0

        lax.fori_loop(0, width, complete, 0)

    half = py < ny // 2

    def last_step(k, _):
        arrived((STEPS - 1) % 2, k)
        chunk(STEPS - 1, k, finish)
        pl.when(half & (k > 0))(lambda: prefix(k - 1))
        return 0

    lax.fori_loop(0, CHUNKS, last_step, 0)
    pl.when(half)(lambda: prefix(CHUNKS - 1))

    @pl.when(jnp.logical_not(half))
    def _():
        def one(k, _):
            prefix(k)
            return 0

        lax.fori_loop(0, CHUNKS, one, 0)

    def drain(k, _):
        sent(0, k)
        sent(1, k)
        pl.when(py < ny - 1)(lambda: pass_on(k).wait_send())
        return 0

    lax.fori_loop(0, CHUNKS, drain, 0)


def solution(mesh):
    sizes = (mesh.shape["py"], mesh.shape["px"], mesh.shape["pz"])

    def local(density, crowding):
        Y, X, Z, S = density.shape
        dma = pltpu.SemaphoreType.DMA
        any_space = pl.BlockSpec(memory_space=pl.ANY)
        vmem = pl.BlockSpec(memory_space=pltpu.VMEM)
        return pl.pallas_call(
            functools.partial(kernel, sizes),
            out_shape=[jax.ShapeDtypeStruct(density.shape, jnp.float32)] * 2,
            in_specs=[any_space, any_space],
            out_specs=[vmem, vmem],
            scratch_shapes=[
                pltpu.VMEM((2, Y + 2, X + 2, Z + 16, S), jnp.float32),
                pltpu.VMEM((Y, X, Z, S), jnp.float32),
                pltpu.VMEM((X, Z, S), jnp.float32),
                pltpu.VMEM((X, Z, S), jnp.float32),
                dma((CHUNKS,)),
                dma((CHUNKS,)),
                dma((2, 2, CHUNKS)),
                dma((2, 2, CHUNKS)),
                dma((2, 2, CHUNKS)),
                dma((2, 2, CHUNKS)),
                dma((2, 2)),
                dma((2, 2)),
                dma((CHUNKS,)),
                dma((CHUNKS,)),
            ],
            compiler_params=pltpu.CompilerParams(
                collective_id=0, has_side_effects=True, vmem_limit_bytes=67_000_000
            ),
        )(density, crowding)

    spec = P("py", "px", "pz", None)
    return jax.shard_map(local, mesh=mesh, in_specs=(spec, spec), out_specs=(spec, spec), check_vma=False)
```

```python
import functools

import jax
import jax.numpy as jnp
from jax import lax
from jax.experimental import pallas as pl
from jax.experimental.pallas import tpu as pltpu
from jax.sharding import PartitionSpec as P

STEPS = 6
CHUNKS = 8
FORWARD_AT = 2
MESH = pl.DeviceIdType.MESH
LOW, HIGH = 8, 40


def kernel(sizes, d_ref, c_ref, col_ref, end_ref, field, crowd, below, total,
           hop, in_sem, c_sem, y_send, y_recv, z_send, z_recv, x_send, x_recv, t_send, t_recv,
           far_send, far_recv, hop_recv, relay_send):
    ny, nx, nz = sizes
    py, px, pz = lax.axis_index("py"), lax.axis_index("px"), lax.axis_index("pz")
    Y, X, Z, _ = d_ref.shape
    width = X // CHUNKS
    upward = lax.rem(px, 2) == 1
    half_x = nx // 2
    part = Y // half_x
    near = (px == half_x - 1) | (px == half_x)
    lane = jnp.where(px < half_x, half_x - 1 - px, px - half_x)
    beside = {"py": py, "px": jnp.where(px < half_x, half_x - 1, half_x), "pz": pz}
    across = {"py": py, "px": jnp.where(px < half_x, half_x, half_x - 1), "pz": pz}

    def start_of(k):
        return pl.multiple_of(jnp.where(upward, k, CHUNKS - 1 - k) * width, width)

    y_up = (py < ny - 1, {"py": py + 1, "px": px, "pz": pz})
    y_down = (py > 0, {"py": py - 1, "px": px, "pz": pz})
    z_up = (pz < nz - 1, {"py": py, "px": px, "pz": pz + 1})
    z_down = (pz > 0, {"py": py, "px": px, "pz": pz - 1})
    first = jnp.where(upward, px - 1, px + 1)
    last = jnp.where(upward, px + 1, px - 1)
    x_first = ((first >= 0) & (first < nx), {"py": py, "px": first, "pz": pz})
    x_last = ((last >= 0) & (last < nx) & jnp.logical_not(near), {"py": py, "px": last, "pz": pz})
    neighbours = (y_up, y_down, z_up, z_down, x_first, x_last)

    def load(k):
        x0 = start_of(k)
        return (
            pltpu.make_async_copy(
                d_ref.at[:, pl.ds(x0, width)],
                field.at[0, pl.ds(1, Y), pl.ds(1 + x0, width), pl.ds(LOW, Z)],
                in_sem.at[k],
            ),
            pltpu.make_async_copy(c_ref.at[:, pl.ds(x0, width)], crowd.at[:, pl.ds(x0, width)], c_sem.at[k]),
        )

    for k in range(CHUNKS):
        load(k)[0].start()
    for k in range(CHUNKS):
        load(k)[1].start()

    barrier = pltpu.get_barrier_semaphore()
    count = 0
    for exists, device in neighbours:
        count = count + exists.astype(jnp.int32)

        @pl.when(exists)
        def _():
            pl.semaphore_signal(barrier, inc=1, device_id=device, device_id_type=MESH)

    ends_of_face = tuple({"py": py, "px": half_x - 1 + i, "pz": pz} for i in range(2))
    relays = tuple({"py": py, "px": x, "pz": pz} for x in range(nx) if x not in (half_x - 1, half_x))
    count = count + jnp.where(near, len(relays) + 1, len(ends_of_face))

    @pl.when(near)
    def _():
        for device in (*relays, across):
            pl.semaphore_signal(barrier, inc=1, device_id=device, device_id_type=MESH)

    @pl.when(jnp.logical_not(near))
    def _():
        for device in ends_of_face:
            pl.semaphore_signal(barrier, inc=1, device_id=device, device_id_type=MESH)

    pl.semaphore_wait(barrier, count)

    def remote(src, dst, send, recv, device):
        return pltpu.make_async_remote_copy(src, dst, send, recv, device_id=device, device_id_type=MESH)

    def faces(p, k):
        xs = pl.ds(1 + start_of(k), width)
        ys, zs = pl.ds(1, Y), pl.ds(LOW, Z)
        f = field.at[p]
        return (
            (y_up[0], remote(f.at[Y, xs, zs], f.at[0, xs, zs], y_send.at[p, 0, k], y_recv.at[p, 0, k], y_up[1])),
            (y_down[0], remote(f.at[1, xs, zs], f.at[Y + 1, xs, zs], y_send.at[p, 1, k], y_recv.at[p, 1, k], y_down[1])),
            (z_up[0], remote(f.at[ys, xs, pl.ds(HIGH - 1, 1)], f.at[ys, xs, pl.ds(LOW - 1, 1)], z_send.at[p, 0, k], z_recv.at[p, 0, k], z_up[1])),
            (z_down[0], remote(f.at[ys, xs, pl.ds(LOW, 1)], f.at[ys, xs, pl.ds(HIGH, 1)], z_send.at[p, 1, k], z_recv.at[p, 1, k], z_down[1])),
        )

    def ends(p, side):
        ys, zs = pl.ds(1, Y), pl.ds(LOW, Z)
        f = field.at[p]
        low = upward if side == 0 else jnp.logical_not(upward)
        src, dst = jnp.where(low, 1, X), jnp.where(low, X + 1, 0)
        exists, device = x_first if side == 0 else x_last
        return exists, remote(f.at[ys, pl.ds(src, 1), zs], f.at[ys, pl.ds(dst, 1), zs], x_send.at[p, side], x_recv.at[p, side], device)

    def part_of(p, x, which):
        return field.at[p, pl.ds(1 + which * part, part), pl.ds(x, 1), pl.ds(LOW, Z)]

    def far(t, which):
        p = t % 2
        low = px == half_x
        src, dst = jnp.where(low, 1, X), jnp.where(low, X + 1, 0)
        if which == 0:
            return remote(part_of(p, src, 0), part_of(p, dst, 0), far_send.at[p, 0], far_recv.at[p, 0], across)
        relay = {"py": py, "px": jnp.where(low, half_x - 1 - which, half_x + which), "pz": pz}
        return remote(part_of(p, src, which), hop.at[t], far_send.at[p, which], hop_recv.at[t], relay)

    def far_in(t, which):
        p = t % 2
        x = jnp.where(px == half_x, 0, X + 1)
        return remote(part_of(p, x, which), part_of(p, x, which), far_send.at[p, which], far_recv.at[p, which], across)

    def onward(t):
        p = t % 2
        dst = part_of(p, jnp.where(px < half_x, X + 1, 0), lane)
        return remote(hop.at[t], dst, relay_send.at[t], far_recv.at[p, lane], beside)

    def forward(t, k):
        @pl.when(jnp.logical_not(near) & (k == FORWARD_AT))
        def _():
            copy = onward(t)
            remote(hop.at[t], hop.at[t], relay_send.at[t], hop_recv.at[t], across).wait_recv()
            copy.start()

    def each(p, k, do_faces, do_ends):
        arrivals = (1, 0, 3, 2)
        fs = faces(p, k)
        for i, (exists, copy) in enumerate(fs):
            do_faces(exists, copy, fs[arrivals[i]][0])
        for side, at in ((0, 0), (1, CHUNKS - 1)):
            exists, copy = ends(p, side)
            pl.when(exists & (k == at))(lambda copy=copy: do_ends(copy))

    def send(t, k):
        each(t % 2, k, lambda e, c, _: pl.when(e)(lambda: c.start()), lambda c: c.start())

        @pl.when(near & (k == CHUNKS - 1))
        def _():
            for which in range(half_x):
                far(t, which).start()

    def sent(t, k):
        each(t % 2, k, lambda e, c, _: pl.when(e)(lambda: c.wait_send()), lambda c: c.wait_send())

        @pl.when(near & (k == CHUNKS - 1))
        def _():
            for which in range(half_x):
                far(t, which).wait_send()

    def arrived(t, k):
        each(t % 2, k, lambda _, c, e: pl.when(e)(lambda: c.wait_recv()), lambda c: c.wait_recv())

        @pl.when(near & (k == CHUNKS - 1))
        def _():
            for which in range(half_x):
                far_in(t, which).wait_recv()

    def cells(p, y, x, z):
        return field[p, y, x, pl.ds(z, 8), :]

    def chunk(t, k, store):
        p = t % 2
        x0 = start_of(k)

        def column(i, _):
            x = x0 + i
            for z in range(LOW, HIGH, 8):
                line = [cells(p, y, 1 + x, z) for y in range(Y + 2)]
                out = []
                for y in range(1, Y + 1):
                    middle = line[y]
                    crowding = crowd[y - 1, x, pl.ds(z - LOW, 8), :]
                    near = (line[y - 1] + line[y + 1]) + (cells(p, y, x, z) + cells(p, y, x + 2, z))
                    near = near + (cells(p, y, 1 + x, z - 1) + cells(p, y, 1 + x, z + 1))
                    out.append(0.1 * (middle * (6.0 - 2.0 * crowding * middle) + near))
                store(x, z, out)
            return 0

        lax.fori_loop(0, width, column, 0)

    def first_send(k, _):
        load(k)[0].wait()
        send(0, k)
        return 0

    lax.fori_loop(0, CHUNKS, first_send, 0)

    zero_row = jnp.zeros((1, 128), jnp.float32)
    zero_plane = jnp.zeros((Z, 128), jnp.float32)

    def clear_rows(row):
        def one(x, _):
            for p in range(2):
                for y in range(1, Y + 1):
                    field[p, y, 1 + x, pl.ds(row, 1), :] = zero_row
            return 0

        lax.fori_loop(0, X, one, 0)

    def clear_plane(y):
        def one(x, _):
            for p in range(2):
                field[p, y, 1 + x, pl.ds(LOW, Z), :] = zero_plane
            return 0

        lax.fori_loop(0, X, one, 0)

    def clear_column(x):
        for p in range(2):
            for y in range(1, Y + 1):
                field[p, y, x, pl.ds(LOW, Z), :] = zero_plane

    pl.when(pz == 0)(lambda: clear_rows(LOW - 1))
    pl.when(pz == nz - 1)(lambda: clear_rows(HIGH))
    pl.when(py == 0)(lambda: clear_plane(0))
    pl.when(py == ny - 1)(lambda: clear_plane(Y + 1))
    pl.when(px == 0)(lambda: clear_column(0))
    pl.when(px == nx - 1)(lambda: clear_column(X + 1))

    for t in range(STEPS - 1):
        q = (t + 1) % 2

        def store(x, z, out):
            for y in range(Y):
                field[q, 1 + y, 1 + x, pl.ds(z, 8), :] = out[y]

        def step(k, _):
            arrived(t, k)
            if t == 0:
                load(k)[1].wait()
            else:
                sent(t - 1, k)
            chunk(t, k, store)
            send(t + 1, k)
            forward(t, k)
            return 0

        lax.fori_loop(0, CHUNKS, step, 0)

    def finish(x, z, out):
        here = None
        for y in range(Y):
            end_ref[y, x, pl.ds(z - LOW, 8), :] = out[y]
            here = out[y] if here is None else here + out[y]
            col_ref[y, x, pl.ds(z - LOW, 8), :] = here
        total[x, pl.ds(z - LOW, 8), :] = here

    def pass_on(k):
        xs = pl.ds(start_of(k), width)
        return remote(total.at[xs], below.at[xs], t_send.at[k], t_recv.at[k], y_up[1])

    def prefix(k):
        x0 = start_of(k)

        @pl.when(py > 0)
        def _():
            pass_on(k).wait_recv()

            def add(i, _):
                total[x0 + i] = total[x0 + i] + below[x0 + i]
                return 0

            lax.fori_loop(0, width, add, 0)

        @pl.when(py < ny - 1)
        def _():
            pass_on(k).start()

        scale = 1.0 / (Y * ny)

        def complete(i, _):
            lower = jnp.where(py > 0, below[x0 + i], 0.0)
            for y in range(Y):
                col_ref[y, x0 + i] = (col_ref[y, x0 + i] + lower) * scale
            return 0

        lax.fori_loop(0, width, complete, 0)

    half = py < ny // 2

    def last_step(k, _):
        arrived(STEPS - 1, k)
        chunk(STEPS - 1, k, finish)
        forward(STEPS - 1, k)
        pl.when(half & (k > 0))(lambda: prefix(k - 1))
        return 0

    lax.fori_loop(0, CHUNKS, last_step, 0)
    pl.when(half)(lambda: prefix(CHUNKS - 1))

    @pl.when(jnp.logical_not(half))
    def _():
        def one(k, _):
            prefix(k)
            return 0

        lax.fori_loop(0, CHUNKS, one, 0)

    def drain(k, _):
        sent(STEPS - 2, k)
        sent(STEPS - 1, k)
        pl.when(py < ny - 1)(lambda: pass_on(k).wait_send())
        return 0

    lax.fori_loop(0, CHUNKS, drain, 0)

    @pl.when(jnp.logical_not(near))
    def _():
        for t in range(STEPS):
            onward(t).wait_send()


def write_out(col_ref, end_ref, col_out, end_out, sem):
    copies = [
        pltpu.make_async_copy(end_ref.at[y], end_out.at[y], sem.at[0, y]) for y in range(end_ref.shape[0])
    ] + [pltpu.make_async_copy(col_ref.at[y], col_out.at[y], sem.at[1, y]) for y in range(col_ref.shape[0])]
    for copy in copies:
        copy.start()
    for copy in copies:
        copy.wait()


def solution(mesh):
    sizes = (mesh.shape["py"], mesh.shape["px"], mesh.shape["pz"])

    def local(density, crowding):
        Y, X, Z, S = density.shape
        dma = pltpu.SemaphoreType.DMA
        any_space = pl.BlockSpec(memory_space=pl.ANY)
        vmem = pl.BlockSpec(memory_space=pltpu.VMEM)
        column_sum, end = pl.pallas_call(
            functools.partial(kernel, sizes),
            out_shape=[pltpu.VMEM(density.shape, jnp.float32)] * 2,
            in_specs=[any_space, any_space],
            out_specs=[vmem, vmem],
            scratch_shapes=[
                pltpu.VMEM((2, Y + 2, X + 2, Z + 16, S), jnp.float32),
                pltpu.VMEM((Y, X, Z, S), jnp.float32),
                pltpu.VMEM((X, Z, S), jnp.float32),
                pltpu.VMEM((X, Z, S), jnp.float32),
                pltpu.VMEM((STEPS, Y // (sizes[1] // 2), 1, Z, S), jnp.float32),
                dma((CHUNKS,)),
                dma((CHUNKS,)),
                dma((2, 2, CHUNKS)),
                dma((2, 2, CHUNKS)),
                dma((2, 2, CHUNKS)),
                dma((2, 2, CHUNKS)),
                dma((2, 2)),
                dma((2, 2)),
                dma((CHUNKS,)),
                dma((CHUNKS,)),
                dma((2, sizes[1] // 2)),
                dma((2, sizes[1] // 2)),
                dma((STEPS,)),
                dma((STEPS,)),
            ],
            compiler_params=pltpu.CompilerParams(
                collective_id=0, has_side_effects=True, vmem_limit_bytes=45_500_000
            ),
        )(density, crowding)
        return pl.pallas_call(
            write_out,
            out_shape=[jax.ShapeDtypeStruct(density.shape, jnp.float32)] * 2,
            in_specs=[vmem, vmem],
            out_specs=[any_space, any_space],
            scratch_shapes=[dma((2, Y))],
            compiler_params=pltpu.CompilerParams(vmem_limit_bytes=4_000_000),
        )(column_sum, end)

    spec = P("py", "px", "pz", None)
    return jax.shard_map(local, mesh=mesh, in_specs=(spec, spec), out_specs=(spec, spec), check_vma=False)
```

```python
import functools

import jax
import jax.numpy as jnp
from jax import lax
from jax.experimental import pallas as pl
from jax.experimental.pallas import tpu as pltpu
from jax.sharding import PartitionSpec as P

STEPS = 6
CHUNKS = 8
FORWARD_AT = 2
MESH = pl.DeviceIdType.MESH
LOW, HIGH = 8, 40


def kernel(sizes, d_ref, c_ref, col_ref, end_ref, field, crowd, below, total,
           hop, in_sem, c_sem, y_send, y_recv, z_send, z_recv, x_send, x_recv, t_send, t_recv,
           far_send, far_recv, hop_recv, relay_send):
    ny, nx, nz = sizes
    py, px, pz = lax.axis_index("py"), lax.axis_index("px"), lax.axis_index("pz")
    Y, X, Z, _ = d_ref.shape
    width = X // CHUNKS
    upward = lax.rem(px, 2) == 1
    half_x = nx // 2
    part = Y // half_x
    near = (px == half_x - 1) | (px == half_x)
    lane = jnp.where(px < half_x, half_x - 1 - px, px - half_x)
    beside = {"py": py, "px": jnp.where(px < half_x, half_x - 1, half_x), "pz": pz}
    across = {"py": py, "px": jnp.where(px < half_x, half_x, half_x - 1), "pz": pz}

    def start_of(k):
        return pl.multiple_of(jnp.where(upward, k, CHUNKS - 1 - k) * width, width)

    y_up = (py < ny - 1, {"py": py + 1, "px": px, "pz": pz})
    y_down = (py > 0, {"py": py - 1, "px": px, "pz": pz})
    z_up = (pz < nz - 1, {"py": py, "px": px, "pz": pz + 1})
    z_down = (pz > 0, {"py": py, "px": px, "pz": pz - 1})
    first = jnp.where(upward, px - 1, px + 1)
    last = jnp.where(upward, px + 1, px - 1)
    x_first = ((first >= 0) & (first < nx), {"py": py, "px": first, "pz": pz})
    x_last = ((last >= 0) & (last < nx) & jnp.logical_not(near), {"py": py, "px": last, "pz": pz})
    neighbours = (y_up, y_down, z_up, z_down, x_first, x_last)

    def load(k):
        x0 = start_of(k)
        return (
            pltpu.make_async_copy(
                d_ref.at[:, pl.ds(x0, width)],
                field.at[0, pl.ds(1, Y), pl.ds(1 + x0, width), pl.ds(LOW, Z)],
                in_sem.at[k],
            ),
            pltpu.make_async_copy(c_ref.at[:, pl.ds(x0, width)], crowd.at[:, pl.ds(x0, width)], c_sem.at[k]),
        )

    barrier = pltpu.get_barrier_semaphore()
    count = 0
    for exists, device in neighbours:
        count = count + exists.astype(jnp.int32)

        @pl.when(exists)
        def _():
            pl.semaphore_signal(barrier, inc=1, device_id=device, device_id_type=MESH)

    ends_of_face = tuple({"py": py, "px": half_x - 1 + i, "pz": pz} for i in range(2))
    relays = tuple({"py": py, "px": x, "pz": pz} for x in range(nx) if x not in (half_x - 1, half_x))
    count = count + jnp.where(near, len(relays) + 1, len(ends_of_face))

    @pl.when(near)
    def _():
        for device in (*relays, across):
            pl.semaphore_signal(barrier, inc=1, device_id=device, device_id_type=MESH)

    @pl.when(jnp.logical_not(near))
    def _():
        for device in ends_of_face:
            pl.semaphore_signal(barrier, inc=1, device_id=device, device_id_type=MESH)

    for k in range(CHUNKS):
        load(k)[0].start()
    pl.semaphore_wait(barrier, count)

    def remote(src, dst, send, recv, device):
        return pltpu.make_async_remote_copy(src, dst, send, recv, device_id=device, device_id_type=MESH)

    def faces(p, k):
        xs = pl.ds(1 + start_of(k), width)
        ys, zs = pl.ds(1, Y), pl.ds(LOW, Z)
        f = field.at[p]
        return (
            (y_up[0], remote(f.at[Y, xs, zs], f.at[0, xs, zs], y_send.at[p, 0, k], y_recv.at[p, 0, k], y_up[1])),
            (y_down[0], remote(f.at[1, xs, zs], f.at[Y + 1, xs, zs], y_send.at[p, 1, k], y_recv.at[p, 1, k], y_down[1])),
            (z_up[0], remote(f.at[ys, xs, pl.ds(HIGH - 1, 1)], f.at[ys, xs, pl.ds(LOW - 1, 1)], z_send.at[p, 0, k], z_recv.at[p, 0, k], z_up[1])),
            (z_down[0], remote(f.at[ys, xs, pl.ds(LOW, 1)], f.at[ys, xs, pl.ds(HIGH, 1)], z_send.at[p, 1, k], z_recv.at[p, 1, k], z_down[1])),
        )

    def ends(p, side):
        ys, zs = pl.ds(1, Y), pl.ds(LOW, Z)
        f = field.at[p]
        low = upward if side == 0 else jnp.logical_not(upward)
        src, dst = jnp.where(low, 1, X), jnp.where(low, X + 1, 0)
        exists, device = x_first if side == 0 else x_last
        return exists, remote(f.at[ys, pl.ds(src, 1), zs], f.at[ys, pl.ds(dst, 1), zs], x_send.at[p, side], x_recv.at[p, side], device)

    def part_of(p, x, which):
        return field.at[p, pl.ds(1 + which * part, part), pl.ds(x, 1), pl.ds(LOW, Z)]

    def far(t, which):
        p = t % 2
        low = px == half_x
        src, dst = jnp.where(low, 1, X), jnp.where(low, X + 1, 0)
        if which == 0:
            return remote(part_of(p, src, 0), part_of(p, dst, 0), far_send.at[p, 0], far_recv.at[p, 0], across)
        relay = {"py": py, "px": jnp.where(low, half_x - 1 - which, half_x + which), "pz": pz}
        return remote(part_of(p, src, which), hop.at[t], far_send.at[p, which], hop_recv.at[t], relay)

    def far_in(t, which):
        p = t % 2
        x = jnp.where(px == half_x, 0, X + 1)
        return remote(part_of(p, x, which), part_of(p, x, which), far_send.at[p, which], far_recv.at[p, which], across)

    def onward(t):
        p = t % 2
        dst = part_of(p, jnp.where(px < half_x, X + 1, 0), lane)
        return remote(hop.at[t], dst, relay_send.at[t], far_recv.at[p, lane], beside)

    def forward(t, k):
        @pl.when(jnp.logical_not(near) & (k == FORWARD_AT))
        def _():
            copy = onward(t)
            remote(hop.at[t], hop.at[t], relay_send.at[t], hop_recv.at[t], across).wait_recv()
            copy.start()

    def each(p, k, do_faces, do_ends):
        arrivals = (1, 0, 3, 2)
        fs = faces(p, k)
        for i, (exists, copy) in enumerate(fs):
            do_faces(exists, copy, fs[arrivals[i]][0])
        for side, at in ((0, 0), (1, CHUNKS - 1)):
            exists, copy = ends(p, side)
            pl.when(exists & (k == at))(lambda copy=copy: do_ends(copy))

    def send(t, k):
        each(t % 2, k, lambda e, c, _: pl.when(e)(lambda: c.start()), lambda c: c.start())

        @pl.when(near & (k == CHUNKS - 1))
        def _():
            for which in range(half_x):
                far(t, which).start()

    def sent(t, k):
        each(t % 2, k, lambda e, c, _: pl.when(e)(lambda: c.wait_send()), lambda c: c.wait_send())

        @pl.when(near & (k == CHUNKS - 1))
        def _():
            for which in range(half_x):
                far(t, which).wait_send()

    def arrived(t, k):
        each(t % 2, k, lambda _, c, e: pl.when(e)(lambda: c.wait_recv()), lambda c: c.wait_recv())

        @pl.when(near & (k == CHUNKS - 1))
        def _():
            for which in range(half_x):
                far_in(t, which).wait_recv()

    def cells(p, y, x, z):
        return field[p, y, x, pl.ds(z, 8), :]

    def chunk(t, k, store):
        p = t % 2
        x0 = start_of(k)

        def column(i, _):
            x = x0 + i
            for z in range(LOW, HIGH, 8):
                line = [cells(p, y, 1 + x, z) for y in range(Y + 2)]
                out = []
                for y in range(1, Y + 1):
                    middle = line[y]
                    crowding = crowd[y - 1, x, pl.ds(z - LOW, 8), :]
                    near = (line[y - 1] + line[y + 1]) + (cells(p, y, x, z) + cells(p, y, x + 2, z))
                    near = near + (cells(p, y, 1 + x, z - 1) + cells(p, y, 1 + x, z + 1))
                    out.append(0.1 * (middle * (6.0 - 2.0 * crowding * middle) + near))
                store(x, z, out)
            return 0

        lax.fori_loop(0, width, column, 0)

    def first_send(k, _):
        load(k)[0].wait()
        send(0, k)
        return 0

    lax.fori_loop(0, CHUNKS, first_send, 0)
    for k in range(CHUNKS):
        load(k)[1].start()

    zero_row = jnp.zeros((1, 128), jnp.float32)
    zero_plane = jnp.zeros((Z, 128), jnp.float32)

    def clear_rows(row):
        def one(x, _):
            for p in range(2):
                for y in range(1, Y + 1):
                    field[p, y, 1 + x, pl.ds(row, 1), :] = zero_row
            return 0

        lax.fori_loop(0, X, one, 0)

    def clear_plane(y):
        def one(x, _):
            for p in range(2):
                field[p, y, 1 + x, pl.ds(LOW, Z), :] = zero_plane
            return 0

        lax.fori_loop(0, X, one, 0)

    def clear_column(x):
        for p in range(2):
            for y in range(1, Y + 1):
                field[p, y, x, pl.ds(LOW, Z), :] = zero_plane

    pl.when(pz == 0)(lambda: clear_rows(LOW - 1))
    pl.when(pz == nz - 1)(lambda: clear_rows(HIGH))
    pl.when(py == 0)(lambda: clear_plane(0))
    pl.when(py == ny - 1)(lambda: clear_plane(Y + 1))
    pl.when(px == 0)(lambda: clear_column(0))
    pl.when(px == nx - 1)(lambda: clear_column(X + 1))

    for t in range(STEPS - 1):
        q = (t + 1) % 2

        def store(x, z, out):
            for y in range(Y):
                field[q, 1 + y, 1 + x, pl.ds(z, 8), :] = out[y]

        def step(k, _):
            arrived(t, k)
            if t == 0:
                load(k)[1].wait()
            else:
                sent(t - 1, k)
            chunk(t, k, store)
            send(t + 1, k)
            forward(t, k)
            return 0

        lax.fori_loop(0, CHUNKS, step, 0)

    def finish(x, z, out):
        here = None
        for y in range(Y):
            end_ref[y, x, pl.ds(z - LOW, 8), :] = out[y]
            here = out[y] if here is None else here + out[y]
            col_ref[y, x, pl.ds(z - LOW, 8), :] = here
        total[x, pl.ds(z - LOW, 8), :] = here

    def pass_on(k):
        xs = pl.ds(start_of(k), width)
        return remote(total.at[xs], below.at[xs], t_send.at[k], t_recv.at[k], y_up[1])

    def prefix(k):
        x0 = start_of(k)

        @pl.when(py > 0)
        def _():
            pass_on(k).wait_recv()

            def add(i, _):
                total[x0 + i] = total[x0 + i] + below[x0 + i]
                return 0

            lax.fori_loop(0, width, add, 0)

        @pl.when(py < ny - 1)
        def _():
            pass_on(k).start()

        scale = 1.0 / (Y * ny)

        def complete(i, _):
            lower = jnp.where(py > 0, below[x0 + i], 0.0)
            for y in range(Y):
                col_ref[y, x0 + i] = (col_ref[y, x0 + i] + lower) * scale
            return 0

        lax.fori_loop(0, width, complete, 0)

    half = py < ny // 2

    def last_step(k, _):
        arrived(STEPS - 1, k)
        chunk(STEPS - 1, k, finish)
        forward(STEPS - 1, k)
        pl.when(half & (k > 0))(lambda: prefix(k - 1))
        return 0

    lax.fori_loop(0, CHUNKS, last_step, 0)
    pl.when(half)(lambda: prefix(CHUNKS - 1))

    def drain(k, _):
        sent(STEPS - 2, k)
        sent(STEPS - 1, k)
        return 0

    lax.fori_loop(0, CHUNKS, drain, 0)

    @pl.when(jnp.logical_not(near))
    def _():
        for t in range(STEPS):
            onward(t).wait_send()

    @pl.when(jnp.logical_not(half))
    def _():
        def one(k, _):
            prefix(k)
            return 0

        lax.fori_loop(0, CHUNKS, one, 0)

    @pl.when(py < ny - 1)
    def _():
        def out(k, _):
            pass_on(k).wait_send()
            return 0

        lax.fori_loop(0, CHUNKS, out, 0)


def write_out(col_ref, end_ref, col_out, end_out, sem):
    copies = [
        pltpu.make_async_copy(end_ref.at[y], end_out.at[y], sem.at[0, y]) for y in range(end_ref.shape[0])
    ] + [pltpu.make_async_copy(col_ref.at[y], col_out.at[y], sem.at[1, y]) for y in range(col_ref.shape[0])]
    for copy in copies:
        copy.start()
    for copy in copies:
        copy.wait()


def solution(mesh):
    sizes = (mesh.shape["py"], mesh.shape["px"], mesh.shape["pz"])

    def local(density, crowding):
        Y, X, Z, S = density.shape
        dma = pltpu.SemaphoreType.DMA
        any_space = pl.BlockSpec(memory_space=pl.ANY)
        vmem = pl.BlockSpec(memory_space=pltpu.VMEM)
        column_sum, end = pl.pallas_call(
            functools.partial(kernel, sizes),
            out_shape=[pltpu.VMEM(density.shape, jnp.float32)] * 2,
            in_specs=[any_space, any_space],
            out_specs=[vmem, vmem],
            scratch_shapes=[
                pltpu.VMEM((2, Y + 2, X + 2, Z + 16, S), jnp.float32),
                pltpu.VMEM((Y, X, Z, S), jnp.float32),
                pltpu.VMEM((X, Z, S), jnp.float32),
                pltpu.VMEM((X, Z, S), jnp.float32),
                pltpu.VMEM((STEPS, Y // (sizes[1] // 2), 1, Z, S), jnp.float32),
                dma((CHUNKS,)),
                dma((CHUNKS,)),
                dma((2, 2, CHUNKS)),
                dma((2, 2, CHUNKS)),
                dma((2, 2, CHUNKS)),
                dma((2, 2, CHUNKS)),
                dma((2, 2)),
                dma((2, 2)),
                dma((CHUNKS,)),
                dma((CHUNKS,)),
                dma((2, sizes[1] // 2)),
                dma((2, sizes[1] // 2)),
                dma((STEPS,)),
                dma((STEPS,)),
            ],
            compiler_params=pltpu.CompilerParams(
                collective_id=0, has_side_effects=True, vmem_limit_bytes=45_500_000
            ),
        )(density, crowding)
        return pl.pallas_call(
            write_out,
            out_shape=[jax.ShapeDtypeStruct(density.shape, jnp.float32)] * 2,
            in_specs=[vmem, vmem],
            out_specs=[any_space, any_space],
            scratch_shapes=[dma((2, Y))],
            compiler_params=pltpu.CompilerParams(vmem_limit_bytes=4_000_000),
        )(column_sum, end)

    spec = P("py", "px", "pz", None)
    return jax.shard_map(local, mesh=mesh, in_specs=(spec, spec), out_specs=(spec, spec), check_vma=False)
```

```python
import functools

import jax
import jax.numpy as jnp
from jax import lax
from jax.experimental import pallas as pl
from jax.experimental.pallas import tpu as pltpu
from jax.sharding import PartitionSpec as P

STEPS = 6
CHUNKS = 8
FORWARD_AT = 3
MESH = pl.DeviceIdType.MESH
LOW, HIGH = 8, 40


def kernel(sizes, d_ref, c_ref, col_ref, end_ref, field, crowd, below, total,
           hop, in_sem, c_sem, y_send, y_recv, z_send, z_recv, x_send, x_recv, t_send, t_recv,
           far_send, far_recv, hop_recv, relay_send):
    ny, nx, nz = sizes
    py, px, pz = lax.axis_index("py"), lax.axis_index("px"), lax.axis_index("pz")
    Y, X, Z, _ = d_ref.shape
    width = X // CHUNKS
    upward = lax.rem(px, 2) == 1
    half_x = nx // 2
    part = Y // half_x
    near = (px == half_x - 1) | (px == half_x)
    lane = jnp.where(px < half_x, half_x - 1 - px, px - half_x)
    beside = {"py": py, "px": jnp.where(px < half_x, half_x - 1, half_x), "pz": pz}
    across = {"py": py, "px": jnp.where(px < half_x, half_x, half_x - 1), "pz": pz}

    def start_of(k):
        return pl.multiple_of(jnp.where(upward, k, CHUNKS - 1 - k) * width, width)

    y_up = (py < ny - 1, {"py": py + 1, "px": px, "pz": pz})
    y_down = (py > 0, {"py": py - 1, "px": px, "pz": pz})
    z_up = (pz < nz - 1, {"py": py, "px": px, "pz": pz + 1})
    z_down = (pz > 0, {"py": py, "px": px, "pz": pz - 1})
    first = jnp.where(upward, px - 1, px + 1)
    last = jnp.where(upward, px + 1, px - 1)
    x_first = ((first >= 0) & (first < nx), {"py": py, "px": first, "pz": pz})
    x_last = ((last >= 0) & (last < nx) & jnp.logical_not(near), {"py": py, "px": last, "pz": pz})
    neighbours = (y_up, y_down, z_up, z_down, x_first, x_last)

    def load(k):
        x0 = start_of(k)
        return (
            pltpu.make_async_copy(
                d_ref.at[:, pl.ds(x0, width)],
                field.at[0, pl.ds(1, Y), pl.ds(1 + x0, width), pl.ds(LOW, Z)],
                in_sem.at[k],
            ),
            pltpu.make_async_copy(c_ref.at[:, pl.ds(x0, width)], crowd.at[:, pl.ds(x0, width)], c_sem.at[k]),
        )

    barrier = pltpu.get_barrier_semaphore()
    count = 0
    for exists, device in neighbours:
        count = count + exists.astype(jnp.int32)

        @pl.when(exists)
        def _():
            pl.semaphore_signal(barrier, inc=1, device_id=device, device_id_type=MESH)

    ends_of_face = tuple({"py": py, "px": half_x - 1 + i, "pz": pz} for i in range(2))
    relays = tuple({"py": py, "px": x, "pz": pz} for x in range(nx) if x not in (half_x - 1, half_x))
    count = count + jnp.where(near, len(relays) + 1, len(ends_of_face))

    @pl.when(near)
    def _():
        for device in (*relays, across):
            pl.semaphore_signal(barrier, inc=1, device_id=device, device_id_type=MESH)

    @pl.when(jnp.logical_not(near))
    def _():
        for device in ends_of_face:
            pl.semaphore_signal(barrier, inc=1, device_id=device, device_id_type=MESH)

    for k in range(CHUNKS):
        load(k)[0].start()
    pl.semaphore_wait(barrier, count)

    def remote(src, dst, send, recv, device):
        return pltpu.make_async_remote_copy(src, dst, send, recv, device_id=device, device_id_type=MESH)

    def faces(p, k):
        xs = pl.ds(1 + start_of(k), width)
        ys, zs = pl.ds(1, Y), pl.ds(LOW, Z)
        f = field.at[p]
        return (
            (y_up[0], remote(f.at[Y, xs, zs], f.at[0, xs, zs], y_send.at[p, 0, k], y_recv.at[p, 0, k], y_up[1])),
            (y_down[0], remote(f.at[1, xs, zs], f.at[Y + 1, xs, zs], y_send.at[p, 1, k], y_recv.at[p, 1, k], y_down[1])),
            (z_up[0], remote(f.at[ys, xs, pl.ds(HIGH - 1, 1)], f.at[ys, xs, pl.ds(LOW - 1, 1)], z_send.at[p, 0, k], z_recv.at[p, 0, k], z_up[1])),
            (z_down[0], remote(f.at[ys, xs, pl.ds(LOW, 1)], f.at[ys, xs, pl.ds(HIGH, 1)], z_send.at[p, 1, k], z_recv.at[p, 1, k], z_down[1])),
        )

    def ends(p, side):
        ys, zs = pl.ds(1, Y), pl.ds(LOW, Z)
        f = field.at[p]
        low = upward if side == 0 else jnp.logical_not(upward)
        src, dst = jnp.where(low, 1, X), jnp.where(low, X + 1, 0)
        exists, device = x_first if side == 0 else x_last
        return exists, remote(f.at[ys, pl.ds(src, 1), zs], f.at[ys, pl.ds(dst, 1), zs], x_send.at[p, side], x_recv.at[p, side], device)

    def part_of(p, x, which):
        return field.at[p, pl.ds(1 + which * part, part), pl.ds(x, 1), pl.ds(LOW, Z)]

    def far(t, which):
        p = t % 2
        low = px == half_x
        src, dst = jnp.where(low, 1, X), jnp.where(low, X + 1, 0)
        if which == 0:
            return remote(part_of(p, src, 0), part_of(p, dst, 0), far_send.at[p, 0], far_recv.at[p, 0], across)
        relay = {"py": py, "px": jnp.where(low, half_x - 1 - which, half_x + which), "pz": pz}
        return remote(part_of(p, src, which), hop.at[t], far_send.at[p, which], hop_recv.at[t], relay)

    def far_in(t, which):
        p = t % 2
        x = jnp.where(px == half_x, 0, X + 1)
        return remote(part_of(p, x, which), part_of(p, x, which), far_send.at[p, which], far_recv.at[p, which], across)

    def onward(t):
        p = t % 2
        dst = part_of(p, jnp.where(px < half_x, X + 1, 0), lane)
        return remote(hop.at[t], dst, relay_send.at[t], far_recv.at[p, lane], beside)

    def forward(t, k):
        @pl.when(jnp.logical_not(near) & (k == FORWARD_AT))
        def _():
            copy = onward(t)
            remote(hop.at[t], hop.at[t], relay_send.at[t], hop_recv.at[t], across).wait_recv()
            copy.start()

    def each(p, k, do_faces, do_ends):
        arrivals = (1, 0, 3, 2)
        fs = faces(p, k)
        for i, (exists, copy) in enumerate(fs):
            do_faces(exists, copy, fs[arrivals[i]][0])
        for side, at in ((0, 0), (1, CHUNKS - 1)):
            exists, copy = ends(p, side)
            pl.when(exists & (k == at))(lambda copy=copy: do_ends(copy))

    def send(t, k):
        each(t % 2, k, lambda e, c, _: pl.when(e)(lambda: c.start()), lambda c: c.start())

        @pl.when(near & (k == CHUNKS - 1))
        def _():
            for which in range(half_x):
                far(t, which).start()

    def sent(t, k):
        each(t % 2, k, lambda e, c, _: pl.when(e)(lambda: c.wait_send()), lambda c: c.wait_send())

        @pl.when(near & (k == CHUNKS - 1))
        def _():
            for which in range(half_x):
                far(t, which).wait_send()

    def arrived(t, k):
        each(t % 2, k, lambda _, c, e: pl.when(e)(lambda: c.wait_recv()), lambda c: c.wait_recv())

        @pl.when(near & (k == CHUNKS - 1))
        def _():
            for which in range(half_x):
                far_in(t, which).wait_recv()

    def cells(p, y, x, z):
        return field[p, y, x, pl.ds(z, 8), :]

    def chunk(t, k, store):
        p = t % 2
        x0 = start_of(k)

        def column(i, _):
            x = x0 + i
            for z in range(LOW, HIGH, 8):
                line = [cells(p, y, 1 + x, z) for y in range(Y + 2)]
                out = []
                for y in range(1, Y + 1):
                    middle = line[y]
                    crowding = crowd[y - 1, x, pl.ds(z - LOW, 8), :]
                    near = (line[y - 1] + line[y + 1]) + (cells(p, y, x, z) + cells(p, y, x + 2, z))
                    near = near + (cells(p, y, 1 + x, z - 1) + cells(p, y, 1 + x, z + 1))
                    out.append(0.1 * (middle * (6.0 - 2.0 * crowding * middle) + near))
                store(x, z, out)
            return 0

        lax.fori_loop(0, width, column, 0)

    def first_send(k, _):
        load(k)[0].wait()
        send(0, k)
        return 0

    lax.fori_loop(0, CHUNKS, first_send, 0)
    for k in range(CHUNKS):
        load(k)[1].start()

    zero_row = jnp.zeros((1, 128), jnp.float32)
    zero_plane = jnp.zeros((Z, 128), jnp.float32)

    def clear_rows(row):
        def one(x, _):
            for p in range(2):
                for y in range(1, Y + 1):
                    field[p, y, 1 + x, pl.ds(row, 1), :] = zero_row
            return 0

        lax.fori_loop(0, X, one, 0)

    def clear_plane(y):
        def one(x, _):
            for p in range(2):
                field[p, y, 1 + x, pl.ds(LOW, Z), :] = zero_plane
            return 0

        lax.fori_loop(0, X, one, 0)

    def clear_column(x):
        for p in range(2):
            for y in range(1, Y + 1):
                field[p, y, x, pl.ds(LOW, Z), :] = zero_plane

    pl.when(pz == 0)(lambda: clear_rows(LOW - 1))
    pl.when(pz == nz - 1)(lambda: clear_rows(HIGH))
    pl.when(py == 0)(lambda: clear_plane(0))
    pl.when(py == ny - 1)(lambda: clear_plane(Y + 1))
    pl.when(px == 0)(lambda: clear_column(0))
    pl.when(px == nx - 1)(lambda: clear_column(X + 1))

    for t in range(STEPS - 1):
        q = (t + 1) % 2

        def store(x, z, out):
            for y in range(Y):
                field[q, 1 + y, 1 + x, pl.ds(z, 8), :] = out[y]

        def step(k, _):
            arrived(t, k)
            if t == 0:
                load(k)[1].wait()
            else:
                sent(t - 1, k)
            chunk(t, k, store)
            send(t + 1, k)
            forward(t, k)
            return 0

        lax.fori_loop(0, CHUNKS, step, 0)

    def finish(x, z, out):
        here = None
        for y in range(Y):
            end_ref[y, x, pl.ds(z - LOW, 8), :] = out[y]
            here = out[y] if here is None else here + out[y]
            col_ref[y, x, pl.ds(z - LOW, 8), :] = here
        total[x, pl.ds(z - LOW, 8), :] = here

    def pass_on(k):
        xs = pl.ds(start_of(k), width)
        return remote(total.at[xs], below.at[xs], t_send.at[k], t_recv.at[k], y_up[1])

    def prefix(k):
        x0 = start_of(k)

        @pl.when(py > 0)
        def _():
            pass_on(k).wait_recv()

            def add(i, _):
                total[x0 + i] = total[x0 + i] + below[x0 + i]
                return 0

            @pl.when(py < ny - 1)
            def _():
                lax.fori_loop(0, width, add, 0)

        @pl.when(py < ny - 1)
        def _():
            pass_on(k).start()

        scale = 1.0 / (Y * ny)

        def complete(i, _):
            lower = jnp.where(py > 0, below[x0 + i], 0.0)
            for y in range(Y):
                col_ref[y, x0 + i] = (col_ref[y, x0 + i] + lower) * scale
            return 0

        lax.fori_loop(0, width, complete, 0)

    half = py < ny // 2

    def last_step(k, _):
        arrived(STEPS - 1, k)
        chunk(STEPS - 1, k, finish)
        forward(STEPS - 1, k)
        pl.when(half & (k > 0))(lambda: prefix(k - 1))
        return 0

    lax.fori_loop(0, CHUNKS, last_step, 0)
    pl.when(half)(lambda: prefix(CHUNKS - 1))

    def drain(k, _):
        sent(STEPS - 2, k)
        sent(STEPS - 1, k)
        return 0

    lax.fori_loop(0, CHUNKS, drain, 0)

    @pl.when(jnp.logical_not(near))
    def _():
        for t in range(STEPS):
            onward(t).wait_send()

    @pl.when(jnp.logical_not(half))
    def _():
        def one(k, _):
            prefix(k)
            return 0

        lax.fori_loop(0, CHUNKS, one, 0)

    @pl.when(py < ny - 1)
    def _():
        def out(k, _):
            pass_on(k).wait_send()
            return 0

        lax.fori_loop(0, CHUNKS, out, 0)


def write_out(col_ref, end_ref, col_out, end_out, sem):
    copies = [
        pltpu.make_async_copy(end_ref.at[y], end_out.at[y], sem.at[0, y]) for y in range(end_ref.shape[0])
    ] + [pltpu.make_async_copy(col_ref.at[y], col_out.at[y], sem.at[1, y]) for y in range(col_ref.shape[0])]
    for copy in copies:
        copy.start()
    for copy in copies:
        copy.wait()


def solution(mesh):
    sizes = (mesh.shape["py"], mesh.shape["px"], mesh.shape["pz"])

    def local(density, crowding):
        Y, X, Z, S = density.shape
        dma = pltpu.SemaphoreType.DMA
        any_space = pl.BlockSpec(memory_space=pl.ANY)
        vmem = pl.BlockSpec(memory_space=pltpu.VMEM)
        column_sum, end = pl.pallas_call(
            functools.partial(kernel, sizes),
            out_shape=[pltpu.VMEM(density.shape, jnp.float32)] * 2,
            in_specs=[any_space, any_space],
            out_specs=[vmem, vmem],
            scratch_shapes=[
                pltpu.VMEM((2, Y + 2, X + 2, Z + 16, S), jnp.float32),
                pltpu.VMEM((Y, X, Z, S), jnp.float32),
                pltpu.VMEM((X, Z, S), jnp.float32),
                pltpu.VMEM((X, Z, S), jnp.float32),
                pltpu.VMEM((STEPS, Y // (sizes[1] // 2), 1, Z, S), jnp.float32),
                dma((CHUNKS,)),
                dma((CHUNKS,)),
                dma((2, 2, CHUNKS)),
                dma((2, 2, CHUNKS)),
                dma((2, 2, CHUNKS)),
                dma((2, 2, CHUNKS)),
                dma((2, 2)),
                dma((2, 2)),
                dma((CHUNKS,)),
                dma((CHUNKS,)),
                dma((2, sizes[1] // 2)),
                dma((2, sizes[1] // 2)),
                dma((STEPS,)),
                dma((STEPS,)),
            ],
            compiler_params=pltpu.CompilerParams(
                collective_id=0, has_side_effects=True, vmem_limit_bytes=45_500_000
            ),
        )(density, crowding)
        return pl.pallas_call(
            write_out,
            out_shape=[jax.ShapeDtypeStruct(density.shape, jnp.float32)] * 2,
            in_specs=[vmem, vmem],
            out_specs=[any_space, any_space],
            scratch_shapes=[dma((2, Y))],
            compiler_params=pltpu.CompilerParams(vmem_limit_bytes=4_000_000),
        )(column_sum, end)

    spec = P("py", "px", "pz", None)
    return jax.shard_map(local, mesh=mesh, in_specs=(spec, spec), out_specs=(spec, spec), check_vma=False)
```
